32 devices in a mesh: dp: 4 (over x, y), tp: 8 (over z, core).
Axes of the slice: x: 2, y: 2, z: 4, core: 2. Of those that a mesh axis runs over, the one named last changes fastest.
Arguments:
- x: bfloat16 [8192, 5120], P(('dp', 'tp')), parts along dimension 0
- gain: bfloat16 [5120], replicated
- wq: bfloat16 [5120, 12288], P(None, 'tp')
- wk: bfloat16 [5120, 1024], P(None, 'tp')
- wv: bfloat16 [5120, 1024], P(None, 'tp')
- wo: bfloat16 [12288, 5120], P('tp')
Outputs:
- output: bfloat16 [8192, 5120], P(('dp', 'tp')), parts along dimension 0
There are 4 independent parts. The reference program is written for one: setup_inputs(seed, part) draws one part's arguments, and reference() takes and returns one part's arrays. A program takes and returns all parts, laid end to end along the dimension named above; an argument that names none is the same for every part.
All inputs are finite; a program needn't handle non-finite values.
Results may differ from the reference program's by a relative error of at most 0.012.
Values are sent between devices in bfloat16 or wider.
A program may use at most 2 GiB of HBM per device.

```python
import jax
import jax.numpy as jnp
from jax import lax

ROWS = 2048
D = 5120
HEADS = 96
KV_HEADS = 8
HEAD = 128
THETA = 10000


def setup_inputs(seed: int = 0, part: int = 0) -> dict:
    kx, kn, kq, kk, kv, ko = jax.random.split(jax.random.key(seed), 6)

    def weights(key, rows, columns):
        return jax.random.normal(key, (rows, columns), jnp.float32) * rows**-0.5

    drawn = {
        "x": jax.random.normal(jax.random.fold_in(kx, part), (ROWS, D), jnp.float32),
        "gain": 1 + 0.1 * jax.random.normal(kn, (D,), jnp.float32),
        "wq": 2 * weights(kq, D, HEADS * HEAD),
        "wk": 2 * weights(kk, D, KV_HEADS * HEAD),
        "wv": 4 * weights(kv, D, KV_HEADS * HEAD),
        "wo": weights(ko, HEADS * HEAD, D),
    }
    return {k: v.astype(jnp.bfloat16) for k, v in drawn.items()}


def normed(x, gain):
    wide = x.astype(jnp.float32)
    scale = lax.rsqrt(jnp.mean(wide * wide, -1, keepdims=True) + 1e-6)
    return (wide * scale * gain.astype(jnp.float32)).astype(jnp.bfloat16)


def turned(t, place, theta):
    half = t.shape[-1] // 2
    angle = place.astype(jnp.float32)[:, None] * theta ** (-jnp.arange(half, dtype=jnp.float32) / half)
    cos, sin = jnp.cos(angle)[:, None], jnp.sin(angle)[:, None]
    a, b = t[..., :half].astype(jnp.float32), t[..., half:].astype(jnp.float32)
    return jnp.concatenate([a * cos - b * sin, b * cos + a * sin], -1).astype(jnp.bfloat16)


def matmul(a, w):
    return jnp.dot(a, w, preferred_element_type=jnp.float32).astype(jnp.bfloat16)


def einsum(form, a, b):
    return jnp.einsum(form, a.astype(jnp.float32), b.astype(jnp.float32))


def attention(q, k, v):
    scores = einsum("tgsd,ugd->gstu", q, k) * q.shape[-1] ** -0.5
    token = jnp.arange(q.shape[0])
    scores = jnp.where(token[:, None] >= token, scores, -jnp.inf)
    weights = jax.nn.softmax(scores, -1).astype(jnp.bfloat16)
    return einsum("gstu,ugd->tgsd", weights, v).astype(jnp.bfloat16)


def reference(x, gain, wq, wk, wv, wo):
    a, place = normed(x, gain), jnp.arange(ROWS)
    q = turned(matmul(a, wq).reshape(ROWS, HEADS, HEAD), place, THETA).reshape(ROWS, KV_HEADS, -1, HEAD)
    k = turned(matmul(a, wk).reshape(ROWS, KV_HEADS, HEAD), place, THETA)
    v = matmul(a, wv).reshape(ROWS, KV_HEADS, HEAD)
    seen = attention(q, k, v).reshape(ROWS, HEADS * HEAD)
    return (x.astype(jnp.float32) + jnp.dot(seen, wo, preferred_element_type=jnp.float32)).astype(jnp.bfloat16)
```

```python
import jax
import jax.numpy as jnp
from jax import lax
from jax.experimental import pallas as pl
from jax.experimental.pallas import tpu as pltpu
from jax.sharding import PartitionSpec as P

NEG = -1e30
HIDDEN = 2 * NEG
LOG2E = 1.4426950408889634
HEAD = 128
THETA = 10000
D = 5120
ROWS = 2048
HEADS = 12
BLOCK = 256
WIDE = HEADS * BLOCK
KEYS = 512
STRIP = 512
NT = 4
TILE = D // NT
FINE = 256
OFF = 1000
BF, F32 = jnp.bfloat16, jnp.float32

BLOCKS = [[0, 1, 2, 4, 6, 8, 10, 12], [2, 4, 5, 6, 7, 8, 9, 10], [3, 5, 7, 9, 10, 11, 12, 13], [4, 6, 8, 10, 12, 14, 15, 16]]
RIGHT = [[OFF, 5, 9, 13], [OFF, OFF, 10, 14], [OFF, OFF, OFF, 15], [OFF] * 4]
LEFT = [[OFF] * 4, [12, OFF, OFF, OFF], [8, 12, OFF, OFF], [7, 11, 15, OFF]]
LAST = [14, 14, 17, 17]
TICKS = 21


def _dot(a, b, ca=1, cb=0):
    return lax.dot_general(a, b, (((ca,), (cb,)), ((), ())), preferred_element_type=F32)


def _kernel(xn, x, cs, wq, wk, wv, wo, y, xall, sibt, ups, wq_v, wkv_v, wo_v, xb, cs_v, kc, vt, qb, seen, gap, top, mix, tbuf, obuf,
            s_v, u_v, x_v, y_v, w_sem, l_sem, ag_r, ag_s, agl_s, sib_r, sib_s, t_r, t_s, u_r, o_s):
    t = lax.axis_index("tp")
    z, c = lax.div(t, 2), lax.rem(t, 2)
    sib, left, right = t + 1 - 2 * c, t - 2, t + 2
    has_l, has_r = z > 0, z < 3
    scale = HEAD**-0.5
    e = scale * LOG2E

    def pick(values):
        r = jnp.int32(values[3])
        for n in (2, 1, 0):
            r = jnp.where(z == n, jnp.int32(values[n]), r)
        return r

    def remote(src, dst, ss, rs, dev):
        return pltpu.make_async_remote_copy(src, dst, ss, rs, device_id={"tp": dev}, device_id_type=pl.DeviceIdType.MESH)

    def signal(dev):
        pl.semaphore_signal(pltpu.get_barrier_semaphore(), inc=1, device_id={"tp": dev}, device_id_type=pl.DeviceIdType.MESH)

    weights = [
        pltpu.make_async_copy(wq, wq_v, w_sem.at[0]),
        pltpu.make_async_copy(wk, wkv_v.at[:, :HEAD], w_sem.at[1]),
        pltpu.make_async_copy(wv, wkv_v.at[:, HEAD:], w_sem.at[2]),
        pltpu.make_async_copy(wo, wo_v, w_sem.at[3]),
    ]
    own_in = pltpu.make_async_copy(xn, xb, l_sem.at[0])
    own_in.start()
    for w in weights:
        w.start()

    signal(sib)
    pl.when(has_l)(lambda: signal(left))
    pl.when(has_r)(lambda: signal(right))
    pl.semaphore_wait(pltpu.get_barrier_semaphore(), 1 + jnp.where(has_l, 1, 0) + jnp.where(has_r, 1, 0))

    def half(row):
        return xall.at[pl.ds(pl.multiple_of(row, 64), 64)]

    def quarter(row):
        return xall.at[pl.ds(pl.multiple_of(row, 128), 128)]

    def swap_own(i, core):
        at = 4 * z + 2 * core + i
        return remote(xn.at[pl.ds(128 * i, 128)], quarter(128 * at), sib_s.at[at], sib_r.at[at], sib)

    def swap(at):
        rows = half(128 * at + 64 * c)
        return remote(rows, rows, sib_s.at[at], sib_r.at[at], sib)

    def onward(at, dev, sem=None):
        rows = half(128 * at + 64 * c)
        return remote(rows, rows, ag_s.at[at] if sem is None else sem, ag_r.at[at], dev)

    swap_own(0, c).start()
    swap_own(1, c).start()
    own_in.wait()
    own_out = pltpu.make_async_copy(xb, xall.at[pl.ds(pl.multiple_of(t * BLOCK, BLOCK), BLOCK)], l_sem.at[1])
    own_out.start()

    gap[...] = lax.rem(lax.broadcasted_iota(jnp.int32, (KEYS, STRIP), 1), BLOCK) - lax.broadcasted_iota(jnp.int32, (KEYS, STRIP), 0)
    kc[...] = jnp.zeros_like(kc)
    vt[...] = jnp.where(lax.broadcasted_iota(jnp.int32, vt.shape, 0) >= HEAD, 1.0, 0.0).astype(BF)

    own_out.wait()
    swap_own(0, 1 - c).wait_recv()
    swap_own(1, 1 - c).wait_recv()
    for p in range(4):
        pl.when(has_l)(lambda: onward(4 * z + p, left, agl_s.at[p]).start())
        pl.when(has_r & (p < z))(lambda: onward(4 * z + p, right).start())
    for w in weights[:3]:
        w.wait()

    def relay(at, dev, more):
        onward(at, dev).wait_recv()
        swap(at).start()
        pl.when(more)(lambda: onward(at, dev).start())

    def turn(acc):
        a = acc.astype(BF).astype(F32)
        return (a * cs_v[:, :HEAD] + pltpu.roll(a, HEAD // 2, 1) * cs_v[:, HEAD:]).astype(BF)

    def attend(j, masked, level):
        keys = pl.ds(pl.multiple_of(j * KEYS, KEYS), KEYS)

        def group(g, _):
            places = [pl.ds(pl.multiple_of((3 * g + i) * STRIP, STRIP), STRIP) for i in range(3)]
            scores = [_dot(kc[keys, :], qb[at, :], 1, 1) for at in places]
            ps, keeps = [], []
            for at, s in zip(places, scores):
                if masked:
                    s = jnp.where(gap[...] >= level, s, HIDDEN)
                old = top[:, at]
                new = jnp.maximum(old, s.max(axis=0, keepdims=True))
                top[:, at] = new
                ps.append(jnp.exp2((s - new) * e).astype(BF))
                keeps.append(jnp.exp2((old - new) * e))
            for at, p, keep in zip(places, ps, keeps):
                mix[:, at] = mix[:, at] * keep + _dot(vt[:, keys], p)
            return 0

        lax.fori_loop(0, WIDE // STRIP // 3, group, 0)

    def block(b):
        j, h = lax.div(b, 2), lax.rem(b, 2)

        @pl.when(j != z)
        def _():
            for i in range(2):
                swap_in = half(128 * (2 * b + i) + 64 * (1 - c))
                remote(swap_in, swap_in, sib_s.at[2 * b + i], sib_r.at[2 * b + i], sib).wait_recv()

        here = pl.ds(pl.multiple_of(b * BLOCK, BLOCK), BLOCK)
        loads = [pltpu.make_async_copy(xall.at[here], xb, l_sem.at[0]), pltpu.make_async_copy(cs.at[here], cs_v, l_sem.at[1])]
        for one in loads:
            one.start()
        for one in loads:
            one.wait()
        kv = _dot(xb[...], wkv_v[...])
        kc[here, :] = turn(kv[:, :HEAD])
        vt[:HEAD, here] = kv[:, HEAD:].T.astype(BF)

        def heads(i, _):
            acc = _dot(xb[...], wq_v[:, pl.ds(pl.multiple_of(i * 256, 256), 256)])
            qb[pl.ds(pl.multiple_of(i * 512, 512), 256), :] = turn(acc[:, :HEAD])
            qb[pl.ds(pl.multiple_of(i * 512 + 256, 256), 256), :] = turn(acc[:, HEAD:])
            return 0

        lax.fori_loop(0, HEADS // 2, heads, 0)
        top[...] = jnp.full_like(top, NEG)
        mix[...] = jnp.zeros_like(mix)

        def whole(i, _):
            attend(i, False, None)
            return 0

        lax.fori_loop(0, j, whole, 0)
        attend(j, True, -BLOCK * h)

        def out(n, _):
            at = pl.ds(pl.multiple_of(n * BLOCK, BLOCK), BLOCK)
            seen[b, :, pl.ds(pl.multiple_of(n * HEAD, HEAD), HEAD)] = (mix[:HEAD, at] * (1 / mix[HEAD : HEAD + 1, at])).T.astype(BF)
            return 0

        lax.fori_loop(0, HEADS, out, 0)

    def fine(n, i):
        return pl.ds(pl.multiple_of(n * TILE + i * FINE, FINE), FINE)

    def share_copy(j, n):
        return remote(tbuf.at[lax.rem(n, 2)], sibt.at[j, n], t_s.at[j, n], t_r.at[j, n], sib)

    def share(j):
        b = 2 * j + 1 - c

        def tile(n, _):
            pl.when(n >= 2)(lambda: share_copy(j, n - 2).wait_send())
            pl.when((n < 2) & (j > 0))(lambda: share_copy(j - 1, n + 2).wait_send())
            for i in range(TILE // FINE):
                tbuf[lax.rem(n, 2), :, i * FINE : (i + 1) * FINE] = _dot(seen[b], wo_v[:, fine(n, i)]).astype(BF)
            share_copy(j, n).start()
            return 0

        lax.fori_loop(0, NT, tile, 0)

    def sum_copy(w, j, n):
        return remote(obuf.at[w, lax.rem(n, 2)], ups.at[w, j, n], o_s.at[j, n], u_r.at[w, j, n], jnp.where(w == 0, right, left))

    def local_in(src, dst, i):
        return pltpu.make_async_copy(src, dst, l_sem.at[i])

    def pass_on(w, j, n):
        b = 2 * j + c
        more = jnp.where(w == 0, z, 3 - z) > 0
        first = jnp.where(w == 0, z + 1, 0)
        pl.when(n >= 2)(lambda: sum_copy(w, j, n - 2).wait_send())
        pl.when((n < 2) & (j > first))(lambda: sum_copy(w, j - 1, n + 2).wait_send())
        share_copy(j, n).wait_recv()
        local_in(sibt.at[j, n], s_v, 0).start()

        @pl.when(more)
        def _():
            sum_copy(w, j, n).wait_recv()
            local_in(ups.at[w, j, n], u_v.at[0], 1).start()
            local_in(ups.at[w, j, n], u_v.at[0], 1).wait()

        local_in(sibt.at[j, n], s_v, 0).wait()
        for i in range(TILE // FINE):
            cols = slice(i * FINE, (i + 1) * FINE)
            acc = _dot(seen[b], wo_v[:, fine(n, i)]) + s_v[:, cols].astype(F32)
            acc = acc + jnp.where(more, u_v[0, :, cols].astype(F32), 0.0)
            obuf[w, lax.rem(n, 2), :, cols] = acc.astype(BF)
        sum_copy(w, j, n).start()

    def finish(n):
        share_copy(z, n).wait_recv()
        cols_out = pl.ds(pl.multiple_of(n * TILE, TILE), TILE)
        local_in(sibt.at[z, n], s_v, 0).start()
        local_in(x.at[:, cols_out], x_v, 2).start()
        for w, has in ((0, has_l), (1, has_r)):
            @pl.when(has)
            def _():
                sum_copy(w, z, n).wait_recv()
                local_in(ups.at[w, z, n], u_v.at[w], 1).start()
                local_in(ups.at[w, z, n], u_v.at[w], 1).wait()
        local_in(sibt.at[z, n], s_v, 0).wait()
        local_in(x.at[:, cols_out], x_v, 2).wait()
        for i in range(TILE // FINE):
            cols = slice(i * FINE, (i + 1) * FINE)
            acc = _dot(seen[2 * z + c], wo_v[:, fine(n, i)]) + s_v[:, cols].astype(F32)
            acc = acc + jnp.where(has_l, u_v[0, :, cols].astype(F32), 0.0) + jnp.where(has_r, u_v[1, :, cols].astype(F32), 0.0)
            y_v[:, cols] = (x_v[:, cols].astype(F32) + acc).astype(BF)
        out = pltpu.make_async_copy(y_v, y.at[:, cols_out], l_sem.at[3])
        out.start()
        out.wait()

    u_v[...] = jnp.zeros_like(u_v)
    weights[3].wait()
    blocks_at = [pick([BLOCKS[n][b] for n in range(4)]) for b in range(8)]
    sums_at = [[pick([table[n][j] for n in range(4)]) for j in range(4)] for table in (RIGHT, LEFT)]
    last_at = pick(LAST)

    def tick(k, _):
        @pl.when(has_r & (k == 5 * z))
        def _():
            for p in range(4):
                pl.when(p >= z)(lambda: onward(4 * z + p, right).start())

        i, m = k - z, k - 1
        pl.when((i >= 0) & (i < 4 * z))(lambda: relay(i, right, has_r))
        pl.when((m >= 0) & (m < 4 * (3 - z)))(lambda: relay(4 * (z + 1) + m, left, has_l))

        begun = sum(jnp.where(s < k, 1, 0) for s in blocks_at)
        now = sum(jnp.where(s <= k, 1, 0) for s in blocks_at)

        @pl.when(now > begun)
        def _():
            block(begun)
            pl.when(lax.rem(begun, 2) == 1)(lambda: share(lax.div(begun, 2)))

        def way(w, _):
            starts = [jnp.where(w == 0, sums_at[0][j], sums_at[1][j]) for j in range(4)]
            on = [(k >= s) & (k < s + NT) for s in starts]
            j = sum(jnp.where(o, n, 0) for n, o in enumerate(on))
            n = sum(jnp.where(o, k - s, 0) for o, s in zip(on, starts))
            pl.when(on[0] | on[1] | on[2] | on[3])(lambda: pass_on(w, j, n))
            return 0

        lax.fori_loop(0, 2, way, 0)
        pl.when((k >= last_at) & (k < last_at + NT))(lambda: finish(k - last_at))
        return 0

    lax.fori_loop(0, TICKS, tick, 0)

    swap_own(0, c).wait_send()
    swap_own(1, c).wait_send()

    def drain(at, _):
        j = lax.div(at, 4)
        pl.when(j != z)(lambda: swap(at).wait_send())
        pl.when(((j <= z) & has_r) | ((j > z) & has_l))(lambda: onward(at, right).wait_send())
        return 0

    lax.fori_loop(0, 16, drain, 0)
    for p in range(4):
        pl.when(has_l)(lambda: onward(4 * z + p, left, agl_s.at[p]).wait_send())
    for n in (2, 3):
        share_copy(3, n).wait_send()
        pl.when(has_r)(lambda: sum_copy(0, 3, n).wait_send())
        pl.when(has_l)(lambda: sum_copy(1, z - 1, n).wait_send())


def normed(x, gain):
    wide = x.astype(F32)
    scale = lax.rsqrt(jnp.mean(wide * wide, -1, keepdims=True) + 1e-6)
    return (wide * scale * gain.astype(F32)).astype(BF)


def tables():
    half = HEAD // 2
    angle = jnp.arange(ROWS).astype(F32)[:, None] * THETA ** (-jnp.arange(half, dtype=F32) / half)
    cos, sin = jnp.cos(angle), jnp.sin(angle)
    return jnp.concatenate([cos, cos, -sin, sin], 1)


def solution(mesh):
    dma = pltpu.SemaphoreType.DMA
    hbm = pl.BlockSpec(memory_space=pl.ANY)

    def step(x, gain, wq, wk, wv, wo):
        y, *_ = pl.pallas_call(
            _kernel,
            in_specs=[hbm] * 7,
            out_specs=[hbm] * 4,
            out_shape=[
                jax.ShapeDtypeStruct((BLOCK, D), BF),
                jax.ShapeDtypeStruct((ROWS, D), BF),
                jax.ShapeDtypeStruct((4, NT, BLOCK, TILE), BF),
                jax.ShapeDtypeStruct((2, 4, NT, BLOCK, TILE), BF),
            ],
            scratch_shapes=[
                pltpu.VMEM((D, HEADS * HEAD), BF),
                pltpu.VMEM((D, 2 * HEAD), BF),
                pltpu.VMEM((HEADS * HEAD, D), BF),
                pltpu.VMEM((BLOCK, D), BF),
                pltpu.VMEM((BLOCK, 2 * HEAD), F32),
                pltpu.VMEM((ROWS, HEAD), BF),
                pltpu.VMEM((HEAD + 16, ROWS), BF),
                pltpu.VMEM((WIDE, HEAD), BF),
                pltpu.VMEM((8, BLOCK, HEADS * HEAD), BF),
                pltpu.VMEM((KEYS, STRIP), jnp.int32),
                pltpu.VMEM((1, WIDE), F32),
                pltpu.VMEM((HEAD + 16, WIDE), F32),
                pltpu.VMEM((2, BLOCK, TILE), BF),
                pltpu.VMEM((2, 2, BLOCK, TILE), BF),
                pltpu.VMEM((BLOCK, TILE), BF),
                pltpu.VMEM((2, BLOCK, TILE), BF),
                pltpu.VMEM((BLOCK, TILE), BF),
                pltpu.VMEM((BLOCK, TILE), BF),
                dma((4,)),
                dma((4,)),
                dma((16,)),
                dma((16,)),
                dma((4,)),
                dma((16,)),
                dma((16,)),
                dma((4, NT)),
                dma((4, NT)),
                dma((2, 4, NT)),
                dma((4, NT)),
            ],
            compiler_params=pltpu.CompilerParams(collective_id=0, has_side_effects=True, vmem_limit_bytes=67043328),
        )(normed(x, gain), x, tables(), wq, wk, wv, wo)
        return y

    tokens, columns = P(("dp", "tp"), None), P(None, "tp")
    return jax.shard_map(
        step,
        mesh=mesh,
        in_specs=(tokens, P(None), columns, columns, columns, P("tp", None)),
        out_specs=tokens,
        check_vma=False,
    )
```

```python
import jax
import jax.numpy as jnp
import numpy as np
from jax import lax
from jax.experimental import pallas as pl
from jax.experimental.pallas import tpu as pltpu
from jax.sharding import PartitionSpec as P

NEG = -1e30
HIDDEN = 2 * NEG
LOG2E = 1.4426950408889634
HEAD = 128
THETA = 10000
D = 5120
ROWS = 2048
HEADS = 12
BLOCK = 256
WIDE = HEADS * BLOCK
KEYS = 512
STRIP = 512
NT = 4
TILE = D // NT
FINE = 256
OFF = 1000
BF, F32 = jnp.bfloat16, jnp.float32

PROJECT = [[0, 1, 5, 9, 13, 17, 21, 25], [5, 9, 1, 0, 6, 10, 13, 21], [6, 10, 14, 18, 0, 1, 5, 9], [8, 11, 15, 19, 23, 30, 1, 2]]
ATTEND = [[0, 3, 5, 9, 13, 17, 22, 26], [5, 9, 10, 12, 14, 18, 20, 25], [6, 12, 15, 19, 22, 24, 30, 33], [8, 11, 16, 19, 23, 30, 32, 33]]
TERM = [[1, 3, 5, 10, 14, 17, 23, 27], [5, 9, 10, 13, 14, 18, 22, 28], [7, 12, 16, 21, 22, 26, 30, 34], [8, 11, 16, 22, 27, 31, 32, 34]]
SLOT = [[0, 0, 0, 0, 0, 0, 0, 0], [2, 3, 1, 0, 2, 3, 0, 0], [3, 4, 4, 4, 0, 1, 2, 3], [2, 2, 2, 2, 2, 2, 0, 1]]
RIGHT = [[OFF, OFF, 7, 11, 15, 20, 25, 29], [OFF, OFF, OFF, OFF, 16, 21, 25, 30], [OFF, OFF, OFF, OFF, OFF, OFF, 31, 35], [OFF, OFF, OFF, OFF, OFF, OFF, OFF, OFF]]
LEFT = [[OFF, OFF, OFF, OFF, OFF, OFF, OFF, OFF], [23, 27, OFF, OFF, OFF, OFF, OFF, OFF], [13, 18, 24, 29, OFF, OFF, OFF, OFF], [10, 14, 18, 23, 28, 32, OFF, OFF]]
LAST = [[28, 38], [27, 36], [35, 41], [36, 41]]
TICKS = 43


def _dot(a, b, ca=1, cb=0):
    return lax.dot_general(a, b, (((ca,), (cb,)), ((), ())), preferred_element_type=F32)


def _kernel(x, gain, cs, wq, wk, wv, wo, y, xall, term, sibt, ups, fint, wq_v, wkv_v, wo_v, gain_v, xb, cs_v, kc, vt, qb, seen, gap, top,
            mix, tbuf, fbuf, obuf, f_v, s_v, u_v, x_v, w_sem, l_sem, ag_r, ag_s, agl_s, sib_r, sib_s, t_r, t_s, u_r, o_s, e_r, e_s, k_sem):
    t = lax.axis_index("tp")
    z, c = lax.div(t, 2), lax.rem(t, 2)
    sib, left, right = t + 1 - 2 * c, t - 2, t + 2
    has_l, has_r = z > 0, z < 3
    e = HEAD**-0.5 * LOG2E

    def pick(values):
        r = jnp.int32(values[3])
        for n in (2, 1, 0):
            r = jnp.where(z == n, jnp.int32(values[n]), r)
        return r

    def remote(src, dst, ss, rs, dev):
        return pltpu.make_async_remote_copy(src, dst, ss, rs, device_id={"tp": dev}, device_id_type=pl.DeviceIdType.MESH)

    def local(src, dst, i):
        return pltpu.make_async_copy(src, dst, l_sem.at[i])

    def both(copies):
        for one in copies:
            one.start()
        for one in copies:
            one.wait()

    def signal(dev):
        pl.semaphore_signal(pltpu.get_barrier_semaphore(), inc=1, device_id={"tp": dev}, device_id_type=pl.DeviceIdType.MESH)

    weights = [
        pltpu.make_async_copy(wq, wq_v, w_sem.at[0]),
        pltpu.make_async_copy(wk, wkv_v.at[:, :HEAD], w_sem.at[1]),
        pltpu.make_async_copy(wv, wkv_v.at[:, HEAD:], w_sem.at[2]),
        pltpu.make_async_copy(wo, wo_v, w_sem.at[3]),
    ]
    first = [local(x, xb, 0), local(gain, gain_v, 1)]
    for one in first + weights:
        one.start()

    signal(sib)
    pl.when(has_l)(lambda: signal(left))
    pl.when(has_r)(lambda: signal(right))

    for one in first:
        one.wait()

    def norm(i, _):
        rows = pl.ds(pl.multiple_of(i * 32, 32), 32)
        wide = xb[rows, :].astype(F32)
        scale = lax.rsqrt(jnp.mean(wide * wide, -1, keepdims=True) + 1e-6)
        xb[rows, :] = (wide * scale * gain_v[...].astype(F32)).astype(BF)
        return 0

    lax.fori_loop(0, BLOCK // 32, norm, 0)
    own_out = local(xb, xall.at[pl.ds(pl.multiple_of(t * BLOCK, BLOCK), BLOCK)], 0)
    own_out.start()
    pl.semaphore_wait(pltpu.get_barrier_semaphore(), 1 + jnp.where(has_l, 1, 0) + jnp.where(has_r, 1, 0))

    def half(at, core):
        return xall.at[pl.ds(pl.multiple_of(64 * at + 32 * core, 32), 32)]

    def swap_own(i, core):
        at = 8 * z + 4 * core + i
        rows = xall.at[pl.ds(pl.multiple_of(64 * at, 64), 64)]
        return remote(rows, rows, sib_s.at[at], sib_r.at[at], sib)

    def swap(at, core):
        return remote(half(at, core), half(at, core), sib_s.at[at], sib_r.at[at], sib)

    def onward(at, dev, sem=None):
        return remote(half(at, c), half(at, c), ag_s.at[at] if sem is None else sem, ag_r.at[at], dev)

    own_out.wait()
    for i in range(4):
        swap_own(i, c).start()

    gap[...] = lax.broadcasted_iota(jnp.int32, gap.shape, 1) - lax.broadcasted_iota(jnp.int32, gap.shape, 0)
    kc[...] = jnp.zeros_like(kc)
    vt[...] = jnp.where(lax.broadcasted_iota(jnp.int32, vt.shape, 0) >= HEAD, 1.0, 0.0).astype(BF)
    u_v[...] = jnp.zeros_like(u_v)

    for i in range(4):
        swap_own(i, 1 - c).wait_recv()
    for p in range(8):
        pl.when(has_l)(lambda: onward(8 * z + p, left, agl_s.at[p]).start())
        pl.when(has_r & (p < z))(lambda: onward(8 * z + p, right).start())
    for w in weights[:3]:
        w.wait()

    def relay(at, dev, more):
        onward(at, dev).wait_recv()
        pl.when(more)(lambda: onward(at, dev).start())
        swap(at, c).start()

    def slot(b):
        return sum(jnp.where(b == n, pick([SLOT[m][n] for m in range(4)]), 0) for n in range(8))

    def project_loads(b):
        here = pl.ds(pl.multiple_of(b * BLOCK, BLOCK), BLOCK)
        return [local(xall.at[here], xb, 0), local(cs.at[here], cs_v, 1)]

    def fetch_block(b):
        @pl.when(lax.div(b, 2) != z)
        def _():
            for i in range(4):
                swap(4 * b + i, 1 - c).wait_recv()

        for one in project_loads(b):
            one.start()

    def project(b):
        here = pl.ds(pl.multiple_of(b * BLOCK, BLOCK), BLOCK)
        for one in project_loads(b):
            one.wait()
        low = lax.broadcasted_iota(jnp.int32, (BLOCK, HEAD), 1) < HEAD // 2

        def turn(acc):
            a, table = acc.astype(BF).astype(F32), cs_v[...]
            other = pltpu.roll(table, HEAD // 2, 1)
            cos, sin = jnp.where(low, table, other), jnp.where(low, -other, table)
            return (a * cos + pltpu.roll(a, HEAD // 2, 1) * sin).astype(BF)

        kv = _dot(xb[...], wkv_v[...])
        kc[here, :] = turn(kv[:, :HEAD])
        vt[:HEAD, here] = kv[:, HEAD:].T.astype(BF)

        def heads(i, _):
            acc = _dot(xb[...], wq_v[:, pl.ds(pl.multiple_of(i * 512, 512), 512)])
            for n in range(4):
                qb[slot(b), pl.ds(pl.multiple_of(i * 1024 + n * 256, 256), 256), :] = turn(acc[:, n * HEAD : (n + 1) * HEAD])
            return 0

        lax.fori_loop(0, HEADS // 4, heads, 0)

    def some_keys(b, j, length=KEYS, level=None):
        keys = pl.ds(pl.multiple_of(j * KEYS, KEYS), length)

        places = [slice(i, i + STRIP) for i in range(0, WIDE, STRIP)]
        scores = [_dot(kc[keys, :], qb[slot(b), at, :], 1, 1) for at in places]
        ps, keeps = [], []
        for at, s in zip(places, scores):
            if level is not None:
                s = jnp.where(jnp.concatenate([gap[:length]] * (STRIP // BLOCK), 1) >= level, s, HIDDEN)
            old = top[:, at]
            new = jnp.maximum(old, s.max(axis=0, keepdims=True))
            top[:, at] = new
            ps.append(jnp.exp2((s - new) * e).astype(BF))
            keeps.append(jnp.exp2((old - new) * e))
        for at, p, keep in zip(places, ps, keeps):
            mix[:, at] = mix[:, at] * keep + _dot(vt[:, keys], p)

    def attend(b):
        top[...] = jnp.full_like(top, NEG)
        mix[...] = jnp.zeros_like(mix)

        def whole(i, _):
            some_keys(b, i)
            return 0

        lax.fori_loop(0, lax.div(b, 2), whole, 0)
        even = lax.rem(b, 2) == 0
        pl.when(even)(lambda: some_keys(b, lax.div(b, 2), BLOCK, 0))
        pl.when(~even)(lambda: some_keys(b, lax.div(b, 2), KEYS, -BLOCK))

        def out(n, _):
            at = pl.ds(pl.multiple_of(n * BLOCK, BLOCK), BLOCK)
            seen[:, pl.ds(pl.multiple_of(n * HEAD, HEAD), HEAD)] = (mix[:HEAD, at] * (1 / mix[HEAD : HEAD + 1, at])).T.astype(BF)
            return 0

        lax.fori_loop(0, HEADS, out, 0)

    def share(b, n):
        return remote(tbuf.at[n], sibt.at[b, n], t_s.at[b, n], t_r.at[b, n], sib)

    def keep(b, n):
        return pltpu.make_async_copy(fbuf.at[n], term.at[b, n], k_sem.at[n])

    def out_term(b):
        def tile(n, _):
            pl.when(b > 0)(lambda: share(b - 1, n).wait_send())
            for i in range(TILE // FINE):
                cols = slice(i * FINE, (i + 1) * FINE)
                acc = _dot(seen[...], wo_v[:, pl.ds(pl.multiple_of(n * TILE + i * FINE, FINE), FINE)])
                tbuf[n, :, cols] = jnp.where(c == 0, acc[128:], acc[:128]).astype(BF)
                fbuf[n, :, cols] = jnp.where(c == 0, acc[:128], acc[128:])
            share(b, n).start()
            keep(b, n).start()
            return 0

        lax.fori_loop(0, NT, tile, 0)

    def kept(b):
        for n in range(NT):
            keep(b, n).wait()

    def sum_copy(w, b, n):
        return remote(obuf.at[w, n], ups.at[w, b, n], o_s.at[b, n], u_r.at[w, b, n], jnp.where(w == 0, right, left))

    def send_sum(w, b, n, acc):
        first = jnp.where(w == 0, 2 * z + 2, 0)
        pl.when(b > first)(lambda: sum_copy(w, b - 1, n).wait_send())
        obuf[w, n] = acc.astype(BF)
        sum_copy(w, b, n).start()

    def begin_sum(w, b):
        for n in range(NT):
            share(b, n).wait_recv()
            local(sibt.at[b, n], s_v.at[n], 10 + n).start()
        for n in range(NT):
            local(sibt.at[b, n], s_v.at[n], 10 + n).wait()
            send_sum(w, b, n, fbuf[n] + s_v[n].astype(F32))

    def own_terms(w, b, n):
        return [local(term.at[b, n], f_v.at[w], 3 + w), local(sibt.at[b, n], s_v.at[w], 10 + w)]

    def fetch_terms(w, b, n):
        share(b, n).wait_recv()
        for one in own_terms(w, b, n):
            one.start()

    def pass_on(w, b, n):
        sum_copy(w, b, n).wait_recv()
        so_far = local(ups.at[w, b, n], u_v.at[w, 0], 5)
        so_far.start()
        for one in own_terms(w, b, n):
            one.wait()
        so_far.wait()
        send_sum(w, b, n, f_v[w] + s_v[w].astype(F32) + u_v[w, 0].astype(F32))

    def end_copy(n):
        cols = pl.ds(pl.multiple_of(n * TILE, TILE), TILE)
        return remote(xb.at[pl.ds(0, 128), cols], fint.at[n], e_s.at[n], e_r.at[n], sib)

    def place(core, n):
        return pl.ds(pl.multiple_of(128 * core, 128), 128), pl.ds(pl.multiple_of(n * TILE, TILE), TILE)

    def finish(h, n0):
        b = 2 * z + h

        def loads(i):
            n = n0 + i
            some = [local(term.at[b, n], f_v.at[i], 3 + i), local(sibt.at[b, n], s_v.at[i], 10 + i), local(x.at[place(c, n)], x_v.at[i], 6 + i)]
            ins = [(has, local(ups.at[w, b, n], u_v.at[w, i], 14 + 2 * i + w), w) for w, has in ((0, has_l), (1, has_r))]
            return some, ins

        for i in range(2):
            share(b, n0 + i).wait_recv()
            some, ins = loads(i)
            for one in some:
                one.start()
            for has, one, w in ins:
                @pl.when(has)
                def _():
                    sum_copy(w, b, n0 + i).wait_recv()
                    one.start()
        for i in range(2):
            some, ins = loads(i)
            for has, one, w in ins:
                pl.when(has)(lambda: one.wait())
            for one in some:
                one.wait()
            acc = f_v[i] + s_v[i].astype(F32)
            acc = acc + jnp.where(has_l, u_v[0, i].astype(F32), 0.0) + jnp.where(has_r, u_v[1, i].astype(F32), 0.0)

            @pl.when(h == c)
            def _():
                x_v[i] = (x_v[i].astype(F32) + acc).astype(BF)
                local(x_v.at[i], y.at[place(c, n0 + i)], 8 + i).start()

            @pl.when(h != c)
            def _():
                xb[:128, pl.ds(pl.multiple_of((n0 + i) * TILE, TILE), TILE)] = acc.astype(BF)
                end_copy(n0 + i).start()

        @pl.when(h == c)
        def _():
            for i in range(2):
                local(x_v.at[i], y.at[place(c, n0 + i)], 8 + i).wait()

    def finish_other():
        mine = [local(x.at[place(1 - c, n)], tbuf.at[n], 6 + n) for n in range(NT)]
        for n in range(NT):
            share(7, n).wait_send()
            mine[n].start()
        ins = [local(fint.at[n], s_v.at[n], 10 + n) for n in range(NT)]
        outs = [local(xb.at[128:, n * TILE : (n + 1) * TILE], y.at[place(1 - c, n)], 14 + n) for n in range(NT)]
        for n in range(NT):
            end_copy(n).wait_recv()
            ins[n].start()
        for n in range(NT):
            mine[n].wait()
            ins[n].wait()
            cols = slice(n * TILE, (n + 1) * TILE)
            xb[128:, cols] = (tbuf[n].astype(F32) + s_v[n].astype(F32)).astype(BF)
            outs[n].start()
        for one in outs:
            one.wait()

    weights[3].wait()

    def times(table):
        return [pick([table[n][b] for n in range(4)]) for b in range(8)]

    project_at, attend_at, term_at = times(PROJECT), times(ATTEND), times(TERM)
    right_at, left_at = times(RIGHT), times(LEFT)
    last_at = [pick([LAST[n][h] for n in range(4)]) for h in range(2)]

    def now(k, starts, do, length=1, late=0):
        on = [(k >= s + late) & (k < s + late + length) for s in starts]
        which = sum(jnp.where(o, n, 0) for n, o in enumerate(on))
        since = sum(jnp.where(o, k - s - late, 0) for o, s in zip(on, starts))
        hit = on[0]
        for o in on[1:]:
            hit = hit | o
        pl.when(hit)(lambda: do(which, since))

    def tick(k, _):
        i, m = k - z, k - 1
        inner = has_l & has_r

        def gather():
            @pl.when(has_r & (k == 9 * z))
            def _():
                for p in range(8):
                    pl.when(p >= z)(lambda: onward(8 * z + p, right).start())

            pl.when((i >= 0) & (i < 8 * z))(lambda: relay(i, right, has_r))
            pl.when((m >= 0) & (m < 8 * (3 - z)))(lambda: relay(8 * (z + 1) + m, left, has_l))

        now(k, term_at, lambda b, _: kept(b), 1, 1)

        @pl.when(inner)
        def _():
            for w, starts in enumerate((right_at, left_at)):
                now(k, starts, lambda b, n: fetch_terms(w, b, n), NT)
            gather()
            for w, starts in enumerate((right_at, left_at)):
                now(k, starts, lambda b, n: pass_on(w, b, n), NT)

        @pl.when(~inner)
        def _():
            now(k, [jnp.where(z == 0, r, l) for r, l in zip(right_at, left_at)], lambda b, _: begin_sum(jnp.where(z == 0, 0, 1), b))
            gather()

        now(k, last_at, lambda h, since: finish(h, 2 * since), 2)
        now(k, project_at, lambda b, _: project(b))
        now(k, attend_at, lambda b, _: attend(b))
        now(k, term_at, lambda b, _: out_term(b))
        now(k, project_at, lambda b, _: fetch_block(b), 1, -1)
        return 0

    now(jnp.int32(-1), project_at, lambda b, _: fetch_block(b), 1, -1)
    lax.fori_loop(0, TICKS, tick, 0)
    finish_other()

    for i in range(4):
        swap_own(i, c).wait_send()

    def drain(at, _):
        j = lax.div(at, 8)
        pl.when(j != z)(lambda: swap(at, c).wait_send())
        pl.when(((j <= z) & has_r) | ((j > z) & has_l))(lambda: onward(at, right).wait_send())
        return 0

    lax.fori_loop(0, 32, drain, 0)
    for p in range(8):
        pl.when(has_l)(lambda: onward(8 * z + p, left, agl_s.at[p]).wait_send())
    for n in range(NT):
        end_copy(n).wait_send()
        pl.when(has_r)(lambda: sum_copy(0, 7, n).wait_send())
        pl.when(has_l)(lambda: sum_copy(1, 2 * z - 1, n).wait_send())


def tables():
    half = HEAD // 2
    angle = np.arange(ROWS, dtype=np.float64)[:, None] * float(THETA) ** (-np.arange(half) / half)
    return np.concatenate([np.cos(angle), np.sin(angle)], 1).astype(np.float32)


def solution(mesh):
    dma = pltpu.SemaphoreType.DMA
    hbm = pl.BlockSpec(memory_space=pl.ANY)

    def step(x, gain, wq, wk, wv, wo):
        y, *_ = pl.pallas_call(
            _kernel,
            in_specs=[hbm] * 7,
            out_specs=[hbm] * 6,
            out_shape=[
                jax.ShapeDtypeStruct((BLOCK, D), BF),
                jax.ShapeDtypeStruct((ROWS, D), BF),
                jax.ShapeDtypeStruct((8, NT, 128, TILE), F32),
                jax.ShapeDtypeStruct((8, NT, 128, TILE), BF),
                jax.ShapeDtypeStruct((2, 8, NT, 128, TILE), BF),
                jax.ShapeDtypeStruct((NT, 128, TILE), BF),
            ],
            scratch_shapes=[
                pltpu.VMEM((D, HEADS * HEAD), BF),
                pltpu.VMEM((D, 2 * HEAD), BF),
                pltpu.VMEM((HEADS * HEAD, D), BF),
                pltpu.VMEM((1, D), BF),
                pltpu.VMEM((BLOCK, D), BF),
                pltpu.VMEM((BLOCK, HEAD), F32),
                pltpu.VMEM((ROWS, HEAD), BF),
                pltpu.VMEM((HEAD + 16, ROWS), BF),
                pltpu.VMEM((5, WIDE, HEAD), BF),
                pltpu.VMEM((BLOCK, HEADS * HEAD), BF),
                pltpu.VMEM((KEYS, BLOCK), jnp.int32),
                pltpu.VMEM((1, WIDE), F32),
                pltpu.VMEM((HEAD + 16, WIDE), F32),
                pltpu.VMEM((NT, 128, TILE), BF),
                pltpu.VMEM((NT, 128, TILE), F32),
                pltpu.VMEM((2, NT, 128, TILE), BF),
                pltpu.VMEM((2, 128, TILE), F32),
                pltpu.VMEM((NT, 128, TILE), BF),
                pltpu.VMEM((2, 2, 128, TILE), BF),
                pltpu.VMEM((2, 128, TILE), BF),
                dma((4,)),
                dma((18,)),
                dma((32,)),
                dma((32,)),
                dma((8,)),
                dma((32,)),
                dma((32,)),
                dma((8, NT)),
                dma((8, NT)),
                dma((2, 8, NT)),
                dma((8, NT)),
                dma((NT,)),
                dma((NT,)),
                dma((NT,)),
            ],
            compiler_params=pltpu.CompilerParams(collective_id=0, has_side_effects=True, vmem_limit_bytes=67043328),
        )(x, gain[None], tables(), wq, wk, wv, wo)
        return y

    tokens, columns = P(("dp", "tp"), None), P(None, "tp")
    return jax.shard_map(
        step,
        mesh=mesh,
        in_specs=(tokens, P(None), columns, columns, columns, P("tp", None)),
        out_specs=tokens,
        check_vma=False,
    )
```

```python
import jax
import jax.numpy as jnp
import numpy as np
from jax import lax
from jax.experimental import pallas as pl
from jax.experimental.pallas import tpu as pltpu
from jax.sharding import PartitionSpec as P

NEG = -1e30
HIDDEN = 2 * NEG
LOG2E = 1.4426950408889634
HEAD = 128
THETA = 10000
D = 5120
ROWS = 2048
HEADS = 12
BLOCK = 256
WIDE = HEADS * BLOCK
KEYS = 512
STRIP = 512
NT = 4
TILE = D // NT
FINE = 256
OFF = 1000
BF, F32 = jnp.bfloat16, jnp.float32

PROJECT = [[0, 1, 5, 8, 12, 16, 21, 25], [4, 8, 3, 0, 6, 9, 19, 34], [5, 11, 14, 20, 0, 1, 7, 9], [6, 10, 14, 19, 24, 29, 0, 1]]
ATTEND = [[0, 3, 5, 10, 12, 18, 21, 25], [5, 9, 11, 13, 15, 18, 25, 35], [6, 11, 15, 20, 25, 28, 31, 33], [6, 11, 14, 19, 25, 31, 38, 41]]
TERM = [[1, 3, 5, 10, 13, 18, 24, 30], [7, 10, 12, 13, 16, 21, 30, 36], [8, 13, 16, 24, 25, 30, 31, 35], [6, 11, 15, 19, 27, 31, 39, 42]]
FRESH = [[1, 0, 0, 1, 1, 1, 1, 0], [1, 1, 0, 1, 0, 0, 0, 0], [1, 0, 0, 0, 1, 1, 0, 0], [1, 1, 1, 0, 0, 0, 0, 0]]
SLOT = [[0, 0, 0, 0, 0, 0, 0, 0], [2, 3, 1, 0, 2, 4, 0, 0], [2, 4, 4, 4, 0, 1, 2, 3], [2, 2, 2, 2, 2, 2, 0, 1]]
RIGHT = [[OFF, OFF, 6, 12, 16, 20, 25, 31], [OFF, OFF, OFF, OFF, 18, 24, 33, 37], [OFF, OFF, OFF, OFF, OFF, OFF, 33, 38], [OFF, OFF, OFF, OFF, OFF, OFF, OFF, OFF]]
LEFT = [[OFF, OFF, OFF, OFF, OFF, OFF, OFF, OFF], [20, 31, OFF, OFF, OFF, OFF, OFF, OFF], [11, 20, 28, 34, OFF, OFF, OFF, OFF], [7, 12, 16, 23, 29, 38, OFF, OFF]]
LAST = [[35, 38], [38, 43], [38, 40], [40, 44]]
TICKS = 46


def _dot(a, b, ca=1, cb=0):
    return lax.dot_general(a, b, (((ca,), (cb,)), ((), ())), preferred_element_type=F32)


def _kernel(x, gain, cs, wq, wk, wv, wo, y, xall, term, sibt, ups, fint, wq_v, wkv_v, wo_v, gain_v, xb, cs_v, kc, vt, qb, seen, gap, top,
            mix, tbuf, fbuf, obuf, f_v, s_v, u_v, x_v, w_sem, l_sem, ag_r, ag_s, agl_s, sib_r, sib_s, t_r, t_s, u_r, o_s, e_r, e_s, k_sem):
    t = lax.axis_index("tp")
    z, c = lax.div(t, 2), lax.rem(t, 2)
    sib, left, right = t + 1 - 2 * c, t - 2, t + 2
    has_l, has_r = z > 0, z < 3
    e = HEAD**-0.5 * LOG2E

    def pick(values):
        r = jnp.int32(values[3])
        for n in (2, 1, 0):
            r = jnp.where(z == n, jnp.int32(values[n]), r)
        return r

    def remote(src, dst, ss, rs, dev):
        return pltpu.make_async_remote_copy(src, dst, ss, rs, device_id={"tp": dev}, device_id_type=pl.DeviceIdType.MESH)

    def local(src, dst, i):
        return pltpu.make_async_copy(src, dst, l_sem.at[i])

    def both(copies):
        for one in copies:
            one.start()
        for one in copies:
            one.wait()

    def signal(dev):
        pl.semaphore_signal(pltpu.get_barrier_semaphore(), inc=1, device_id={"tp": dev}, device_id_type=pl.DeviceIdType.MESH)

    weights = [
        pltpu.make_async_copy(wq, wq_v, w_sem.at[0]),
        pltpu.make_async_copy(wk, wkv_v.at[:, :HEAD], w_sem.at[1]),
        pltpu.make_async_copy(wv, wkv_v.at[:, HEAD:], w_sem.at[2]),
        pltpu.make_async_copy(wo, wo_v, w_sem.at[3]),
    ]
    first = [local(x.at[pl.ds(64 * i, 64)], xb.at[pl.ds(64 * i, 64)], i) for i in range(4)] + [local(gain, gain_v, 4)]
    for one in first + weights:
        one.start()

    signal(sib)
    pl.when(has_l)(lambda: signal(left))
    pl.when(has_r)(lambda: signal(right))

    first[4].wait()

    def norm(i, _):
        rows = pl.ds(pl.multiple_of(i * 32, 32), 32)
        wide = xb[rows, :].astype(F32)
        scale = lax.rsqrt(jnp.mean(wide * wide, -1, keepdims=True) + 1e-6)
        xb[rows, :] = (wide * scale * gain_v[...].astype(F32)).astype(BF)
        return 0

    def half(at, core):
        return xall.at[pl.ds(pl.multiple_of(64 * at + 32 * core, 32), 32)]

    def swap_own(i, core):
        at = 8 * z + 4 * core + i
        rows = xall.at[pl.ds(pl.multiple_of(64 * at, 64), 64)]
        return remote(rows, rows, sib_s.at[at], sib_r.at[at], sib)

    def swap(at, core):
        return remote(half(at, core), half(at, core), sib_s.at[at], sib_r.at[at], sib)

    def onward(at, dev, sem=None):
        return remote(half(at, c), half(at, c), ag_s.at[at] if sem is None else sem, ag_r.at[at], dev)

    outs = [local(xb.at[pl.ds(64 * i, 64)], xall.at[pl.ds(pl.multiple_of(t * BLOCK + 64 * i, 64), 64)], 10 + i) for i in range(4)]
    pl.semaphore_wait(pltpu.get_barrier_semaphore(), 1 + jnp.where(has_l, 1, 0) + jnp.where(has_r, 1, 0))
    for i in range(5):
        if i < 4:
            first[i].wait()
            lax.fori_loop(2 * i, 2 * i + 2, norm, 0)
            outs[i].start()
        if i > 0:
            outs[i - 1].wait()
            swap_own(i - 1, c).start()

    gap[...] = lax.broadcasted_iota(jnp.int32, gap.shape, 1) - lax.broadcasted_iota(jnp.int32, gap.shape, 0)
    kc[...] = jnp.zeros_like(kc)
    vt[...] = jnp.where(lax.broadcasted_iota(jnp.int32, vt.shape, 0) >= HEAD, 1.0, 0.0).astype(BF)
    u_v[...] = jnp.zeros_like(u_v)

    for p in range(8):
        pl.when(c != p // 4)(lambda: swap_own(p % 4, 1 - c).wait_recv())
        pl.when(has_l)(lambda: onward(8 * z + p, left, agl_s.at[p]).start())
        pl.when(has_r & ((p < z) | (z == 0)))(lambda: onward(8 * z + p, right).start())

    def relay(at, dev, more):
        onward(at, dev).wait_recv()
        pl.when(more)(lambda: onward(at, dev).start())
        swap(at, c).start()

    def slot(b):
        return sum(jnp.where(b == n, pick([SLOT[m][n] for m in range(4)]), 0) for n in range(8))

    def project_loads(b):
        here = pl.ds(pl.multiple_of(b * BLOCK, BLOCK), BLOCK)
        return [local(xall.at[here], xb, 0), local(cs.at[here], cs_v, 1)]

    def fetch_block(b):
        @pl.when(lax.div(b, 2) != z)
        def _():
            for i in range(4):
                swap(4 * b + i, 1 - c).wait_recv()

        for one in project_loads(b):
            one.start()

    def project(b):
        here = pl.ds(pl.multiple_of(b * BLOCK, BLOCK), BLOCK)
        for one in project_loads(b):
            one.wait()
        low = lax.broadcasted_iota(jnp.int32, (BLOCK, HEAD), 1) < HEAD // 2

        def turn(acc):
            a, table = acc.astype(BF).astype(F32), cs_v[...]
            other = pltpu.roll(table, HEAD // 2, 1)
            cos, sin = jnp.where(low, table, other), jnp.where(low, -other, table)
            return (a * cos + pltpu.roll(a, HEAD // 2, 1) * sin).astype(BF)

        kv = _dot(xb[...], wkv_v[...])
        kc[here, :] = turn(kv[:, :HEAD])
        vt[:HEAD, here] = kv[:, HEAD:].T.astype(BF)

        def heads(i, _):
            acc = _dot(xb[...], wq_v[:, pl.ds(pl.multiple_of(i * 512, 512), 512)])
            for n in range(4):
                qb[slot(b), pl.ds(pl.multiple_of(i * 1024 + n * 256, 256), 256), :] = turn(acc[:, n * HEAD : (n + 1) * HEAD])
            return 0

        lax.fori_loop(0, HEADS // 4, heads, 0)

    def some_keys(b, j, length=KEYS, level=None):
        keys = pl.ds(pl.multiple_of(j * KEYS, KEYS), length)

        places = [slice(i, i + STRIP) for i in range(0, WIDE, STRIP)]
        scores = [_dot(kc[keys, :], qb[slot(b), at, :], 1, 1) for at in places]
        ps, keeps = [], []
        for at, s in zip(places, scores):
            if level is not None:
                s = jnp.where(jnp.concatenate([gap[:length]] * (STRIP // BLOCK), 1) >= level, s, HIDDEN)
            old = top[:, at]
            new = jnp.maximum(old, s.max(axis=0, keepdims=True))
            top[:, at] = new
            ps.append(jnp.exp2((s - new) * e).astype(BF))
            keeps.append(jnp.exp2((old - new) * e))
        for at, p, keep in zip(places, ps, keeps):
            mix[:, at] = mix[:, at] * keep + _dot(vt[:, keys], p)

    def attend(b):
        top[...] = jnp.full_like(top, NEG)
        mix[...] = jnp.zeros_like(mix)

        def whole(i, _):
            some_keys(b, i)
            return 0

        lax.fori_loop(0, lax.div(b, 2), whole, 0)
        even = lax.rem(b, 2) == 0
        pl.when(even)(lambda: some_keys(b, lax.div(b, 2), BLOCK, 0))
        pl.when(~even)(lambda: some_keys(b, lax.div(b, 2), KEYS, -BLOCK))

        def out(n, _):
            at = pl.ds(pl.multiple_of(n * BLOCK, BLOCK), BLOCK)
            seen[:, pl.ds(pl.multiple_of(n * HEAD, HEAD), HEAD)] = (mix[:HEAD, at] * (1 / mix[HEAD : HEAD + 1, at])).T.astype(BF)
            return 0

        lax.fori_loop(0, HEADS, out, 0)

    def share(b, n):
        return remote(tbuf.at[n], sibt.at[b, n], t_s.at[b, n], t_r.at[b, n], sib)

    def keep(b, n):
        return pltpu.make_async_copy(fbuf.at[n], term.at[b, n], k_sem.at[n])

    def out_term(b):
        def tile(n, _):
            pl.when(b > 0)(lambda: share(b - 1, n).wait_send())
            for i in range(TILE // FINE):
                cols = slice(i * FINE, (i + 1) * FINE)
                acc = _dot(seen[...], wo_v[:, pl.ds(pl.multiple_of(n * TILE + i * FINE, FINE), FINE)])
                tbuf[n, :, cols] = jnp.where(c == 0, acc[128:], acc[:128]).astype(BF)
                fbuf[n, :, cols] = jnp.where(c == 0, acc[:128], acc[128:])
            share(b, n).start()
            keep(b, n).start()
            return 0

        lax.fori_loop(0, NT, tile, 0)

    def kept(b):
        for n in range(NT):
            keep(b, n).wait()

    def sum_copy(w, b, n):
        return remote(obuf.at[w, n], ups.at[w, b, n], o_s.at[b, n], u_r.at[w, b, n], jnp.where(w == 0, right, left))

    def send_sum(w, b, n, acc):
        first = jnp.where(w == 0, 2 * z + 2, 0)
        pl.when(b > first)(lambda: sum_copy(w, b - 1, n).wait_send())
        obuf[w, n] = acc.astype(BF)
        sum_copy(w, b, n).start()

    def begin_sum(w, b):
        for n in range(NT):
            share(b, n).wait_recv()
            local(sibt.at[b, n], s_v.at[n], 10 + n).start()
        for n in range(NT):
            local(sibt.at[b, n], s_v.at[n], 10 + n).wait()
            send_sum(w, b, n, fbuf[n] + s_v[n].astype(F32))

    def own_terms(w, b, n):
        return [local(term.at[b, n], f_v.at[w], 3 + w), local(sibt.at[b, n], s_v.at[w], 10 + w)]

    def fetch_terms(w, b, n):
        share(b, n).wait_recv()
        for one in own_terms(w, b, n):
            one.start()

    def pass_on(w, b, n):
        sum_copy(w, b, n).wait_recv()
        so_far = local(ups.at[w, b, n], u_v.at[w, 0], 5)
        so_far.start()
        for one in own_terms(w, b, n):
            one.wait()
        so_far.wait()
        send_sum(w, b, n, f_v[w] + s_v[w].astype(F32) + u_v[w, 0].astype(F32))

    def end_copy(n):
        cols = pl.ds(pl.multiple_of(n * TILE, TILE), TILE)
        return remote(xb.at[pl.ds(0, 128), cols], fint.at[n], e_s.at[n], e_r.at[n], sib)

    def place(core, n):
        return pl.ds(pl.multiple_of(128 * core, 128), 128), pl.ds(pl.multiple_of(n * TILE, TILE), TILE)

    def finish(h, n0):
        b = 2 * z + h

        def loads(i):
            n = n0 + i
            some = [local(term.at[b, n], f_v.at[i], 3 + i), local(sibt.at[b, n], s_v.at[i], 10 + i), local(x.at[place(c, n)], x_v.at[i], 6 + i)]
            ins = [(has, local(ups.at[w, b, n], u_v.at[w, i], 14 + 2 * i + w), w) for w, has in ((0, has_l), (1, has_r))]
            return some, ins

        for i in range(2):
            share(b, n0 + i).wait_recv()
            some, ins = loads(i)
            for one in some:
                one.start()
            for has, one, w in ins:
                @pl.when(has)
                def _():
                    sum_copy(w, b, n0 + i).wait_recv()
                    one.start()
        for i in range(2):
            some, ins = loads(i)
            for has, one, w in ins:
                pl.when(has)(lambda: one.wait())
            for one in some:
                one.wait()
            acc = f_v[i] + s_v[i].astype(F32)
            acc = acc + jnp.where(has_l, u_v[0, i].astype(F32), 0.0) + jnp.where(has_r, u_v[1, i].astype(F32), 0.0)

            @pl.when(h == c)
            def _():
                x_v[i] = (x_v[i].astype(F32) + acc).astype(BF)
                local(x_v.at[i], y.at[place(c, n0 + i)], 8 + i).start()

            @pl.when(h != c)
            def _():
                xb[:128, pl.ds(pl.multiple_of((n0 + i) * TILE, TILE), TILE)] = acc.astype(BF)
                end_copy(n0 + i).start()

        @pl.when(h == c)
        def _():
            for i in range(2):
                local(x_v.at[i], y.at[place(c, n0 + i)], 8 + i).wait()

    def finish_other():
        mine = [local(x.at[place(1 - c, n)], tbuf.at[n], 6 + n) for n in range(NT)]
        for n in range(NT):
            share(7, n).wait_send()
            mine[n].start()
        ins = [local(fint.at[n], s_v.at[n], 10 + n) for n in range(NT)]
        outs = [local(xb.at[128:, n * TILE : (n + 1) * TILE], y.at[place(1 - c, n)], 14 + n) for n in range(NT)]
        for n in range(NT):
            end_copy(n).wait_recv()
            ins[n].start()
        for n in range(NT):
            mine[n].wait()
            ins[n].wait()
            cols = slice(n * TILE, (n + 1) * TILE)
            xb[128:, cols] = (tbuf[n].astype(F32) + s_v[n].astype(F32)).astype(BF)
            outs[n].start()
        for one in outs:
            one.wait()


    def times(table):
        return [pick([table[n][b] for n in range(4)]) for b in range(8)]

    project_at, attend_at, term_at = times(PROJECT), times(ATTEND), times(TERM)
    fresh_at, early_at = (times([[a if f == w else OFF for a, f in zip(*row)] for row in zip(PROJECT, FRESH)]) for w in (1, 0))
    right_at, left_at = times(RIGHT), times(LEFT)
    last_at = [pick([LAST[n][h] for n in range(4)]) for h in range(2)]

    def now(k, starts, do, length=1, late=0):
        on = [(k >= s + late) & (k < s + late + length) for s in starts]
        which = sum(jnp.where(o, n, 0) for n, o in enumerate(on))
        since = sum(jnp.where(o, k - s - late, 0) for o, s in zip(on, starts))
        hit = on[0]
        for o in on[1:]:
            hit = hit | o
        pl.when(hit)(lambda: do(which, since))

    def tick(k, _):
        i, m = k - z, k - 1
        inner = has_l & has_r

        def gather():
            @pl.when(inner & (k == 9 * z))
            def _():
                for p in range(8):
                    pl.when(p >= z)(lambda: onward(8 * z + p, right).start())

            pl.when((i >= 0) & (i < 8 * z))(lambda: relay(i, right, has_r))
            pl.when((m >= 0) & (m < 8 * (3 - z)))(lambda: relay(8 * (z + 1) + m, left, has_l))

        now(k, term_at, lambda b, _: kept(b), 1, 1)

        @pl.when(inner)
        def _():
            for w, starts in enumerate((right_at, left_at)):
                now(k, starts, lambda b, n: fetch_terms(w, b, n), NT)
            gather()
            for w, starts in enumerate((right_at, left_at)):
                now(k, starts, lambda b, n: pass_on(w, b, n), NT)

        @pl.when(~inner)
        def _():
            now(k, [jnp.where(z == 0, r, l) for r, l in zip(right_at, left_at)], lambda b, _: begin_sum(jnp.where(z == 0, 0, 1), b))
            gather()

        now(k, last_at, lambda h, since: finish(h, 2 * since), 2)
        @pl.when(k == 0)
        def _():
            for w in weights[:3]:
                w.wait()

        now(k, fresh_at, lambda b, _: fetch_block(b))
        now(k, project_at, lambda b, _: project(b))
        now(k, attend_at, lambda b, _: attend(b))
        now(k, term_at, lambda b, _: out_term(b))
        pl.when(k == 0)(lambda: weights[3].wait())
        now(k, early_at, lambda b, _: fetch_block(b), 1, -1)
        return 0

    now(jnp.int32(-1), early_at, lambda b, _: fetch_block(b), 1, -1)
    lax.fori_loop(0, TICKS, tick, 0)
    finish_other()

    for i in range(4):
        swap_own(i, c).wait_send()

    def drain(at, _):
        j = lax.div(at, 8)
        pl.when(j != z)(lambda: swap(at, c).wait_send())
        pl.when(((j <= z) & has_r) | ((j > z) & has_l))(lambda: onward(at, right).wait_send())
        return 0

    lax.fori_loop(0, 32, drain, 0)
    for p in range(8):
        pl.when(has_l)(lambda: onward(8 * z + p, left, agl_s.at[p]).wait_send())
    for n in range(NT):
        end_copy(n).wait_send()
        pl.when(has_r)(lambda: sum_copy(0, 7, n).wait_send())
        pl.when(has_l)(lambda: sum_copy(1, 2 * z - 1, n).wait_send())


def tables():
    half = HEAD // 2
    angle = np.arange(ROWS, dtype=np.float64)[:, None] * float(THETA) ** (-np.arange(half) / half)
    return np.concatenate([np.cos(angle), np.sin(angle)], 1).astype(np.float32)


def solution(mesh):
    dma = pltpu.SemaphoreType.DMA
    hbm = pl.BlockSpec(memory_space=pl.ANY)

    def step(x, gain, wq, wk, wv, wo):
        y, *_ = pl.pallas_call(
            _kernel,
            in_specs=[hbm] * 7,
            out_specs=[hbm] * 6,
            out_shape=[
                jax.ShapeDtypeStruct((BLOCK, D), BF),
                jax.ShapeDtypeStruct((ROWS, D), BF),
                jax.ShapeDtypeStruct((8, NT, 128, TILE), F32),
                jax.ShapeDtypeStruct((8, NT, 128, TILE), BF),
                jax.ShapeDtypeStruct((2, 8, NT, 128, TILE), BF),
                jax.ShapeDtypeStruct((NT, 128, TILE), BF),
            ],
            scratch_shapes=[
                pltpu.VMEM((D, HEADS * HEAD), BF),
                pltpu.VMEM((D, 2 * HEAD), BF),
                pltpu.VMEM((HEADS * HEAD, D), BF),
                pltpu.VMEM((1, D), BF),
                pltpu.VMEM((BLOCK, D), BF),
                pltpu.VMEM((BLOCK, HEAD), F32),
                pltpu.VMEM((ROWS, HEAD), BF),
                pltpu.VMEM((HEAD + 16, ROWS), BF),
                pltpu.VMEM((5, WIDE, HEAD), BF),
                pltpu.VMEM((BLOCK, HEADS * HEAD), BF),
                pltpu.VMEM((KEYS, BLOCK), jnp.int32),
                pltpu.VMEM((1, WIDE), F32),
                pltpu.VMEM((HEAD + 16, WIDE), F32),
                pltpu.VMEM((NT, 128, TILE), BF),
                pltpu.VMEM((NT, 128, TILE), F32),
                pltpu.VMEM((2, NT, 128, TILE), BF),
                pltpu.VMEM((2, 128, TILE), F32),
                pltpu.VMEM((NT, 128, TILE), BF),
                pltpu.VMEM((2, 2, 128, TILE), BF),
                pltpu.VMEM((2, 128, TILE), BF),
                dma((4,)),
                dma((18,)),
                dma((32,)),
                dma((32,)),
                dma((8,)),
                dma((32,)),
                dma((32,)),
                dma((8, NT)),
                dma((8, NT)),
                dma((2, 8, NT)),
                dma((8, NT)),
                dma((NT,)),
                dma((NT,)),
                dma((NT,)),
            ],
            compiler_params=pltpu.CompilerParams(collective_id=0, has_side_effects=True, vmem_limit_bytes=67043328),
        )(x, gain[None], tables(), wq, wk, wv, wo)
        return y

    tokens, columns = P(("dp", "tp"), None), P(None, "tp")
    return jax.shard_map(
        step,
        mesh=mesh,
        in_specs=(tokens, P(None), columns, columns, columns, P("tp", None)),
        out_specs=tokens,
        check_vma=False,
    )
```

```python
import jax
import jax.numpy as jnp
import numpy as np
from jax import lax
from jax.experimental import pallas as pl
from jax.experimental.pallas import tpu as pltpu
from jax.sharding import PartitionSpec as P

NEG = -1e30
HIDDEN = 2 * NEG
LOG2E = 1.4426950408889634
HEAD = 128
THETA = 10000
D = 5120
ROWS = 2048
HEADS = 12
BLOCK = 256
WIDE = HEADS * BLOCK
KEYS = 512
STRIP = 512
NT = 4
TILE = D // NT
FINE = 256
OFF = 1000
SLOTS = 5
BF, F32 = jnp.bfloat16, jnp.float32

PROJECT = [[0, 2, 5, 8, 12, 16, 21, 26], [4, 8, 1, 0, 7, 10, 13, 20], [5, 11, 14, 21, 0, 1, 7, 10], [6, 10, 14, 20, 23, 30, 4, 0]]
ATTEND = [[0, 3, 5, 8, 12, 16, 21, 26], [5, 9, 12, 13, 16, 21, 27, 30], [6, 11, 14, 21, 24, 27, 35, 37], [6, 11, 14, 21, 23, 30, 33, 40]]
TERM = [[0, 4, 5, 8, 12, 16, 21, 26], [6, 9, 12, 13, 18, 24, 28, 33], [8, 12, 16, 22, 24, 28, 35, 39], [7, 12, 15, 22, 29, 31, 35, 41]]
FRESH = ["11011111", "11000000", "10000000", "11100001"]
RIGHT = [[OFF, OFF, 6, 10, 14, 18, 22, 28], [OFF, OFF, OFF, OFF, 19, 25, 29, 34], [OFF, OFF, OFF, OFF, OFF, OFF, 36, 40], [OFF, OFF, OFF, OFF, OFF, OFF, OFF, OFF]]
LEFT = [[OFF, OFF, OFF, OFF, OFF, OFF, OFF, OFF], [29, 34, OFF, OFF, OFF, OFF, OFF, OFF], [13, 20, 27, 38, OFF, OFF, OFF, OFF], [9, 13, 18, 23, 30, 34, OFF, OFF]]
LAST = [[33, 44], [35, 44], [41, 44], [41, 44]]
TICKS = 46


def places(begun, done):
    busy, place = [-1] * SLOTS, [0] * len(begun)
    for b in sorted(range(len(begun)), key=lambda b: begun[b]):
        place[b] = min(s for s in range(SLOTS) if busy[s] < begun[b])
        busy[place[b]] = done[b]
    return place


def _dot(a, b, ca=1, cb=0):
    return lax.dot_general(a, b, (((ca,), (cb,)), ((), ())), preferred_element_type=F32)


def _kernel(x, gain, cs, wq, wk, wv, wo, y, xall, term, sibt, ups, fint, wq_v, wkv_v, wo_v, gain_v, xb, cs_v, kc, vt, qb, seen, gap, top,
            mix, tbuf, fbuf, obuf, f_v, s_v, u_v, x_v, w_sem, l_sem, ag_r, ag_s, agl_s, sib_r, sib_s, t_r, t_s, u_r, o_s, e_r, e_s, k_sem):
    t = lax.axis_index("tp")
    z, c = lax.div(t, 2), lax.rem(t, 2)
    sib, left, right = t + 1 - 2 * c, t - 2, t + 2
    has_l, has_r = z > 0, z < 3
    e = HEAD**-0.5 * LOG2E

    def pick(values):
        r = jnp.int32(values[3])
        for n in (2, 1, 0):
            r = jnp.where(z == n, jnp.int32(values[n]), r)
        return r

    def remote(src, dst, ss, rs, dev):
        return pltpu.make_async_remote_copy(src, dst, ss, rs, device_id={"tp": dev}, device_id_type=pl.DeviceIdType.MESH)

    def local(src, dst, i):
        return pltpu.make_async_copy(src, dst, l_sem.at[i])

    def both(copies):
        for one in copies:
            one.start()
        for one in copies:
            one.wait()

    def signal(dev):
        pl.semaphore_signal(pltpu.get_barrier_semaphore(), inc=1, device_id={"tp": dev}, device_id_type=pl.DeviceIdType.MESH)

    weights = [
        pltpu.make_async_copy(wq, wq_v, w_sem.at[0]),
        pltpu.make_async_copy(wk, wkv_v.at[:, :HEAD], w_sem.at[1]),
        pltpu.make_async_copy(wv, wkv_v.at[:, HEAD:], w_sem.at[2]),
        pltpu.make_async_copy(wo, wo_v, w_sem.at[3]),
    ]
    first = [local(x.at[pl.ds(64 * i, 64)], xb.at[pl.ds(64 * i, 64)], i) for i in range(4)] + [local(gain, gain_v, 4)]
    for one in first + weights:
        one.start()

    signal(sib)
    pl.when(has_l)(lambda: signal(left))
    pl.when(has_r)(lambda: signal(right))

    first[4].wait()

    def norm(i, _):
        rows = pl.ds(pl.multiple_of(i * 32, 32), 32)
        wide = xb[rows, :].astype(F32)
        scale = lax.rsqrt(jnp.mean(wide * wide, -1, keepdims=True) + 1e-6)
        xb[rows, :] = (wide * scale * gain_v[...].astype(F32)).astype(BF)
        return 0

    def half(at, core):
        return xall.at[pl.ds(pl.multiple_of(64 * at + 32 * core, 32), 32)]

    def swap_own(i, core):
        at = 8 * z + 4 * core + i
        rows = xall.at[pl.ds(pl.multiple_of(64 * at, 64), 64)]
        return remote(rows, rows, sib_s.at[at], sib_r.at[at], sib)

    def swap(at, core):
        return remote(half(at, core), half(at, core), sib_s.at[at], sib_r.at[at], sib)

    def onward(at, dev, sem=None):
        return remote(half(at, c), half(at, c), ag_s.at[at] if sem is None else sem, ag_r.at[at], dev)

    outs = [local(xb.at[pl.ds(64 * i, 64)], xall.at[pl.ds(pl.multiple_of(t * BLOCK + 64 * i, 64), 64)], 10 + i) for i in range(4)]
    pl.semaphore_wait(pltpu.get_barrier_semaphore(), 1 + jnp.where(has_l, 1, 0) + jnp.where(has_r, 1, 0))
    for i in range(5):
        if i < 4:
            first[i].wait()
            lax.fori_loop(2 * i, 2 * i + 2, norm, 0)
            outs[i].start()
        if i > 0:
            outs[i - 1].wait()
            swap_own(i - 1, c).start()

    gap[...] = lax.broadcasted_iota(jnp.int32, gap.shape, 1) - lax.broadcasted_iota(jnp.int32, gap.shape, 0)
    kc[...] = jnp.zeros_like(kc)
    vt[...] = jnp.where(lax.broadcasted_iota(jnp.int32, vt.shape, 0) >= HEAD, 1.0, 0.0).astype(BF)
    u_v[...] = jnp.zeros_like(u_v)

    for p in range(8):
        pl.when(c != p // 4)(lambda: swap_own(p % 4, 1 - c).wait_recv())
        pl.when(has_l)(lambda: onward(8 * z + p, left, agl_s.at[p]).start())
        pl.when(has_r & ((p < z) | (z == 0)))(lambda: onward(8 * z + p, right).start())

    def relay(at, dev, more):
        onward(at, dev).wait_recv()
        pl.when(more)(lambda: onward(at, dev).start())
        swap(at, c).start()

    def slot(b):
        rows = [places(*row) for row in zip(PROJECT, ATTEND)]
        return sum(jnp.where(b == n, pick(list(column)), 0) for n, column in enumerate(zip(*rows)))

    def project_loads(b):
        here = pl.ds(pl.multiple_of(b * BLOCK, BLOCK), BLOCK)
        return [local(xall.at[here], xb, 0), local(cs.at[here], cs_v, 1)]

    def fetch_block(b):
        @pl.when(lax.div(b, 2) != z)
        def _():
            for i in range(4):
                swap(4 * b + i, 1 - c).wait_recv()

        for one in project_loads(b):
            one.start()

    def project(b):
        here = pl.ds(pl.multiple_of(b * BLOCK, BLOCK), BLOCK)
        for one in project_loads(b):
            one.wait()
        low = lax.broadcasted_iota(jnp.int32, (BLOCK, HEAD), 1) < HEAD // 2

        def turn(acc):
            a, table = acc.astype(BF).astype(F32), cs_v[...]
            other = pltpu.roll(table, HEAD // 2, 1)
            cos, sin = jnp.where(low, table, other), jnp.where(low, -other, table)
            return (a * cos + pltpu.roll(a, HEAD // 2, 1) * sin).astype(BF)

        kv = _dot(xb[...], wkv_v[...])
        kc[here, :] = turn(kv[:, :HEAD])
        vt[:HEAD, here] = kv[:, HEAD:].T.astype(BF)

        def heads(i, _):
            acc = _dot(xb[...], wq_v[:, pl.ds(pl.multiple_of(i * 512, 512), 512)])
            for n in range(4):
                qb[slot(b), pl.ds(pl.multiple_of(i * 1024 + n * 256, 256), 256), :] = turn(acc[:, n * HEAD : (n + 1) * HEAD])
            return 0

        lax.fori_loop(0, HEADS // 4, heads, 0)

    def some_keys(b, j, length=KEYS, level=None):
        keys = pl.ds(pl.multiple_of(j * KEYS, KEYS), length)

        places = [slice(i, i + STRIP) for i in range(0, WIDE, STRIP)]
        scores = [_dot(kc[keys, :], qb[slot(b), at, :], 1, 1) for at in places]
        ps, keeps = [], []
        for at, s in zip(places, scores):
            if level is not None:
                s = jnp.where(jnp.concatenate([gap[:length]] * (STRIP // BLOCK), 1) >= level, s, HIDDEN)
            old = top[:, at]
            new = jnp.maximum(old, s.max(axis=0, keepdims=True))
            top[:, at] = new
            ps.append(jnp.exp2((s - new) * e).astype(BF))
            keeps.append(jnp.exp2((old - new) * e))
        for at, p, keep in zip(places, ps, keeps):
            mix[:, at] = mix[:, at] * keep + _dot(vt[:, keys], p)

    def attend(b):
        top[...] = jnp.full_like(top, NEG)
        mix[...] = jnp.zeros_like(mix)

        def whole(i, _):
            some_keys(b, i)
            return 0

        lax.fori_loop(0, lax.div(b, 2), whole, 0)
        even = lax.rem(b, 2) == 0
        pl.when(even)(lambda: some_keys(b, lax.div(b, 2), BLOCK, 0))
        pl.when(~even)(lambda: some_keys(b, lax.div(b, 2), KEYS, -BLOCK))

        def out(n, _):
            at = pl.ds(pl.multiple_of(n * BLOCK, BLOCK), BLOCK)
            seen[:, pl.ds(pl.multiple_of(n * HEAD, HEAD), HEAD)] = (mix[:HEAD, at] * (1 / mix[HEAD : HEAD + 1, at])).T.astype(BF)
            return 0

        lax.fori_loop(0, HEADS, out, 0)

    def share(b, n):
        return remote(tbuf.at[n], sibt.at[b, n], t_s.at[b, n], t_r.at[b, n], sib)

    def keep(b, n):
        return pltpu.make_async_copy(fbuf.at[n], term.at[b, n], k_sem.at[n])

    def out_term(b):
        def tile(n, _):
            pl.when(b > 0)(lambda: share(b - 1, n).wait_send())
            for i in range(TILE // FINE):
                cols = slice(i * FINE, (i + 1) * FINE)
                acc = _dot(seen[...], wo_v[:, pl.ds(pl.multiple_of(n * TILE + i * FINE, FINE), FINE)])
                tbuf[n, :, cols] = jnp.where(c == 0, acc[128:], acc[:128]).astype(BF)
                fbuf[n, :, cols] = jnp.where(c == 0, acc[:128], acc[128:])
            share(b, n).start()
            keep(b, n).start()
            return 0

        lax.fori_loop(0, NT, tile, 0)

    def kept(b):
        for n in range(NT):
            keep(b, n).wait()

    def sum_copy(w, b, n):
        return remote(obuf.at[w, n], ups.at[w, b, n], o_s.at[b, n], u_r.at[w, b, n], jnp.where(w == 0, right, left))

    def send_sum(w, b, n, acc):
        first = jnp.where(w == 0, 2 * z + 2, 0)
        pl.when(b > first)(lambda: sum_copy(w, b - 1, n).wait_send())
        obuf[w, n] = acc.astype(BF)
        sum_copy(w, b, n).start()

    def begin_sum(w, b):
        for n in range(NT):
            share(b, n).wait_recv()
            local(sibt.at[b, n], s_v.at[n], 10 + n).start()
        for n in range(NT):
            local(sibt.at[b, n], s_v.at[n], 10 + n).wait()
            send_sum(w, b, n, fbuf[n] + s_v[n].astype(F32))

    def own_terms(w, b, n):
        return [local(term.at[b, n], f_v.at[w], 3 + w), local(sibt.at[b, n], s_v.at[w], 10 + w)]

    def fetch_terms(w, b, n):
        share(b, n).wait_recv()
        for one in own_terms(w, b, n):
            one.start()

    def pass_on(w, b, n):
        sum_copy(w, b, n).wait_recv()
        so_far = local(ups.at[w, b, n], u_v.at[w, 0], 5)
        so_far.start()
        for one in own_terms(w, b, n):
            one.wait()
        so_far.wait()
        send_sum(w, b, n, f_v[w] + s_v[w].astype(F32) + u_v[w, 0].astype(F32))

    def end_copy(n):
        cols = pl.ds(pl.multiple_of(n * TILE, TILE), TILE)
        return remote(xb.at[pl.ds(0, 128), cols], fint.at[n], e_s.at[n], e_r.at[n], sib)

    def place(core, n):
        return pl.ds(pl.multiple_of(128 * core, 128), 128), pl.ds(pl.multiple_of(n * TILE, TILE), TILE)

    def finish(h, n0):
        b = 2 * z + h

        def loads(i):
            n = n0 + i
            some = [local(term.at[b, n], f_v.at[i], 3 + i), local(sibt.at[b, n], s_v.at[i], 10 + i), local(x.at[place(c, n)], x_v.at[i], 6 + i)]
            ins = [(has, local(ups.at[w, b, n], u_v.at[w, i], 14 + 2 * i + w), w) for w, has in ((0, has_l), (1, has_r))]
            return some, ins

        for i in range(2):
            share(b, n0 + i).wait_recv()
            some, ins = loads(i)
            for one in some:
                one.start()
            for has, one, w in ins:
                @pl.when(has)
                def _():
                    sum_copy(w, b, n0 + i).wait_recv()
                    one.start()
        for i in range(2):
            some, ins = loads(i)
            for has, one, w in ins:
                pl.when(has)(lambda: one.wait())
            for one in some:
                one.wait()
            acc = f_v[i] + s_v[i].astype(F32)
            acc = acc + jnp.where(has_l, u_v[0, i].astype(F32), 0.0) + jnp.where(has_r, u_v[1, i].astype(F32), 0.0)

            @pl.when(h == c)
            def _():
                x_v[i] = (x_v[i].astype(F32) + acc).astype(BF)
                local(x_v.at[i], y.at[place(c, n0 + i)], 8 + i).start()

            @pl.when(h != c)
            def _():
                xb[:128, pl.ds(pl.multiple_of((n0 + i) * TILE, TILE), TILE)] = acc.astype(BF)
                end_copy(n0 + i).start()

        @pl.when(h == c)
        def _():
            for i in range(2):
                local(x_v.at[i], y.at[place(c, n0 + i)], 8 + i).wait()

    def finish_other():
        mine = [local(x.at[place(1 - c, n)], tbuf.at[n], 6 + n) for n in range(NT)]
        for n in range(NT):
            share(7, n).wait_send()
            mine[n].start()
        ins = [local(fint.at[n], s_v.at[n], 10 + n) for n in range(NT)]
        outs = [local(xb.at[128:, n * TILE : (n + 1) * TILE], y.at[place(1 - c, n)], 14 + n) for n in range(NT)]
        for n in range(NT):
            end_copy(n).wait_recv()
            ins[n].start()
        for n in range(NT):
            mine[n].wait()
            ins[n].wait()
            cols = slice(n * TILE, (n + 1) * TILE)
            xb[128:, cols] = (tbuf[n].astype(F32) + s_v[n].astype(F32)).astype(BF)
            outs[n].start()
        for one in outs:
            one.wait()


    def times(table):
        return [pick([table[n][b] for n in range(4)]) for b in range(8)]

    project_at, attend_at, term_at = times(PROJECT), times(ATTEND), times(TERM)
    fresh_at, early_at = (times([[a if f == w else OFF for a, f in zip(*row)] for row in zip(PROJECT, FRESH)]) for w in "10")
    right_at, left_at = times(RIGHT), times(LEFT)
    last_at = [pick([LAST[n][h] for n in range(4)]) for h in range(2)]

    def now(k, starts, do, length=1, late=0):
        on = [(k >= s + late) & (k < s + late + length) for s in starts]
        which = sum(jnp.where(o, n, 0) for n, o in enumerate(on))
        since = sum(jnp.where(o, k - s - late, 0) for o, s in zip(on, starts))
        hit = on[0]
        for o in on[1:]:
            hit = hit | o
        pl.when(hit)(lambda: do(which, since))

    def tick(k, _):
        i, m = k - z, k - 1
        inner = has_l & has_r

        def gather():
            @pl.when(inner & (k == 9 * z))
            def _():
                for p in range(8):
                    pl.when(p >= z)(lambda: onward(8 * z + p, right).start())

            pl.when((i >= 0) & (i < 8 * z))(lambda: relay(i, right, has_r))
            pl.when((m >= 0) & (m < 8 * (3 - z)))(lambda: relay(8 * (z + 1) + m, left, has_l))

        now(k, term_at, lambda b, _: kept(b), 1, 1)

        @pl.when(inner)
        def _():
            for w, starts in enumerate((right_at, left_at)):
                now(k, starts, lambda b, n: fetch_terms(w, b, n), NT)
            gather()
            for w, starts in enumerate((right_at, left_at)):
                now(k, starts, lambda b, n: pass_on(w, b, n), NT)

        @pl.when(~inner)
        def _():
            now(k, [jnp.where(z == 0, r, l) for r, l in zip(right_at, left_at)], lambda b, _: begin_sum(jnp.where(z == 0, 0, 1), b))
            gather()

        now(k, last_at, lambda h, since: finish(h, 2 * since), 2)
        @pl.when(k == 0)
        def _():
            for w in weights[:3]:
                w.wait()

        now(k, fresh_at, lambda b, _: fetch_block(b))
        now(k, project_at, lambda b, _: project(b))
        now(k, attend_at, lambda b, _: attend(b))
        pl.when(k == 0)(lambda: weights[3].wait())
        now(k, term_at, lambda b, _: out_term(b))
        now(k, early_at, lambda b, _: fetch_block(b), 1, -1)
        return 0

    now(jnp.int32(-1), early_at, lambda b, _: fetch_block(b), 1, -1)
    lax.fori_loop(0, TICKS, tick, 0)
    finish_other()

    for i in range(4):
        swap_own(i, c).wait_send()

    def drain(at, _):
        j = lax.div(at, 8)
        pl.when(j != z)(lambda: swap(at, c).wait_send())
        pl.when(((j <= z) & has_r) | ((j > z) & has_l))(lambda: onward(at, right).wait_send())
        return 0

    lax.fori_loop(0, 32, drain, 0)
    for p in range(8):
        pl.when(has_l)(lambda: onward(8 * z + p, left, agl_s.at[p]).wait_send())
    for n in range(NT):
        end_copy(n).wait_send()
        pl.when(has_r)(lambda: sum_copy(0, 7, n).wait_send())
        pl.when(has_l)(lambda: sum_copy(1, 2 * z - 1, n).wait_send())


def tables():
    half = HEAD // 2
    angle = np.arange(ROWS, dtype=np.float64)[:, None] * float(THETA) ** (-np.arange(half) / half)
    return np.concatenate([np.cos(angle), np.sin(angle)], 1).astype(np.float32)


def solution(mesh):
    dma = pltpu.SemaphoreType.DMA
    hbm = pl.BlockSpec(memory_space=pl.ANY)

    def step(x, gain, wq, wk, wv, wo):
        y, *_ = pl.pallas_call(
            _kernel,
            in_specs=[hbm] * 7,
            out_specs=[hbm] * 6,
            out_shape=[
                jax.ShapeDtypeStruct((BLOCK, D), BF),
                jax.ShapeDtypeStruct((ROWS, D), BF),
                jax.ShapeDtypeStruct((8, NT, 128, TILE), F32),
                jax.ShapeDtypeStruct((8, NT, 128, TILE), BF),
                jax.ShapeDtypeStruct((2, 8, NT, 128, TILE), BF),
                jax.ShapeDtypeStruct((NT, 128, TILE), BF),
            ],
            scratch_shapes=[
                pltpu.VMEM((D, HEADS * HEAD), BF),
                pltpu.VMEM((D, 2 * HEAD), BF),
                pltpu.VMEM((HEADS * HEAD, D), BF),
                pltpu.VMEM((1, D), BF),
                pltpu.VMEM((BLOCK, D), BF),
                pltpu.VMEM((BLOCK, HEAD), F32),
                pltpu.VMEM((ROWS, HEAD), BF),
                pltpu.VMEM((HEAD + 16, ROWS), BF),
                pltpu.VMEM((SLOTS, WIDE, HEAD), BF),
                pltpu.VMEM((BLOCK, HEADS * HEAD), BF),
                pltpu.VMEM((KEYS, BLOCK), jnp.int32),
                pltpu.VMEM((1, WIDE), F32),
                pltpu.VMEM((HEAD + 16, WIDE), F32),
                pltpu.VMEM((NT, 128, TILE), BF),
                pltpu.VMEM((NT, 128, TILE), F32),
                pltpu.VMEM((2, NT, 128, TILE), BF),
                pltpu.VMEM((2, 128, TILE), F32),
                pltpu.VMEM((NT, 128, TILE), BF),
                pltpu.VMEM((2, 2, 128, TILE), BF),
                pltpu.VMEM((2, 128, TILE), BF),
                dma((4,)),
                dma((18,)),
                dma((32,)),
                dma((32,)),
                dma((8,)),
                dma((32,)),
                dma((32,)),
                dma((8, NT)),
                dma((8, NT)),
                dma((2, 8, NT)),
                dma((8, NT)),
                dma((NT,)),
                dma((NT,)),
                dma((NT,)),
            ],
            compiler_params=pltpu.CompilerParams(collective_id=0, has_side_effects=True, vmem_limit_bytes=67043328),
        )(x, gain[None], tables(), wq, wk, wv, wo)
        return y

    tokens, columns = P(("dp", "tp"), None), P(None, "tp")
    return jax.shard_map(
        step,
        mesh=mesh,
        in_specs=(tokens, P(None), columns, columns, columns, P("tp", None)),
        out_specs=tokens,
        check_vma=False,
    )
```
